32 devices in a mesh: rep: 2 (over y), seq: 4 (over z), head: 2 (over x), sub: 2 (over core).
Axes of the slice: x: 2, y: 2, z: 4, core: 2. Of those that a mesh axis runs over, the one named last changes fastest.
Arguments:
- queries: bfloat16 [8, 8192], P('rep', 'head'), parts along dimension 0, may hold values from -4.5 to 4.5
- key_cache: bfloat16 [1024, 128, 1024], P(('rep', 'seq', 'sub'), None, 'head'), parts along dimension 0, may hold values from -4.5 to 4.5
- value_cache: bfloat16 [1024, 128, 1024], P(('rep', 'seq', 'sub'), None, 'head'), parts along dimension 0, may hold values from -6 to 6
- seq_lengths: int32 [8], P('rep'), parts along dimension 0, may hold values from 513 to 32768, as said below
- slot_owner: int32 [1024], P(('rep', 'seq', 'sub')), parts along dimension 0, may hold values from 0 to 3, as said below
- slot_page: int32 [1024], P(('rep', 'seq', 'sub')), parts along dimension 0, may hold values from 0 to 255, as said below
- out_weight: bfloat16 [8192, 8192], P('head', ('seq', 'sub')), may hold values from -0.0625 to 0.0625
Outputs:
- projected: bfloat16 [8, 8192], P('rep', ('seq', 'sub')), parts along dimension 0
The draws below stay inside these ranges and needn't reach their ends.
There are 2 independent parts, one for each index of `rep`. The reference program is written for one: setup_inputs(seed, part) draws one part's arguments, and reference() takes and returns one part's arrays. A program takes and returns all parts, laid end to end along the dimension named above; an argument that names none is the same for every part. Nothing has to cross between parts.
Inputs may be any that keep to these rules, and one draw needn't show every extreme that they name: `slot_owner`: every sequence holds 5 to 256 pages, and some sequence exactly 256; its pages are numbered 0 upward and each stands in exactly one cache page; every cache page is used; a sequence's pages occupy consecutive cache pages. slot_page[s] < ceil(seq_lengths[slot_owner[s]] / 128), and every page below that count is present. seq_lengths[b] lies in the last of its sequence's pages.
All inputs are finite; a program needn't handle non-finite values.
Results may differ from the reference program's by a relative error of at most 0.0055.
Values may be sent and summed in bfloat16 or wider, within the bound.
A program may use at most 64 MiB of HBM per device.

```python
import jax
import jax.numpy as jnp
from jax import lax

D = 8192
HQ = 64
KVH = 8
DH = 128
PAGE = 128
PAGE_DEV = 64
SLOTS = 512
BATCH = 4
MAX_PAGES = 256


min_pages = 5


def page_layout(key):
    longest = jax.random.randint(jax.random.fold_in(key, 13), (), 0, BATCH).astype(jnp.int32)
    indices = jnp.arange(BATCH, dtype=jnp.int32)
    others = (indices != longest).astype(jnp.int32)
    roots = jax.random.randint(jax.random.fold_in(key, 11), (BATCH,), 1, 8).astype(jnp.int32)
    weights = roots * roots * roots * others
    spare = SLOTS - MAX_PAGES - (BATCH - 1) * min_pages
    room_cap = MAX_PAGES - min_pages
    extra = spare * weights // jnp.sum(weights)
    extra = jnp.minimum(extra, room_cap) * others
    leftover = spare - jnp.sum(extra)
    room = (room_cap - extra) * others
    before = jnp.cumsum(room) - room
    extra = extra + jnp.clip(leftover - before, 0, room)
    pages = jnp.where(others == 1, min_pages + extra, MAX_PAGES).astype(jnp.int32)
    ends = jnp.cumsum(pages).astype(jnp.int32)
    starts = ends - pages
    slot_index = jnp.arange(SLOTS, dtype=jnp.int32)
    owners = jnp.sum((slot_index[:, None] >= ends[None, :]).astype(jnp.int32), axis=1).astype(jnp.int32)
    page_number = (slot_index - starts[owners]).astype(jnp.int32)
    tails = jax.random.randint(jax.random.fold_in(key, 12), (BATCH,), 1, PAGE + 1).astype(jnp.int32)
    tails = jnp.where(others == 1, tails, PAGE)
    lengths = ((pages - 1) * PAGE + tails).astype(jnp.int32)
    return (lengths, owners, page_number)


def draw_seq_lengths(key, part):
    return page_layout(key)[0]


def draw_slot_owner(key, part):
    return page_layout(key)[1]


def draw_slot_page(key, part):
    return page_layout(key)[2]


def draw_queries(key, part):
    values = jnp.clip(jax.random.normal(jax.random.fold_in(key, 41), (BATCH, HQ * DH), jnp.float32), -4.5, 4.5)
    return values.astype(jnp.bfloat16)


def draw_key_cache(key, part):
    values = jnp.clip(jax.random.normal(jax.random.fold_in(key, 51), (SLOTS, PAGE, KVH * DH), jnp.float32), -4.5, 4.5)
    return values.astype(jnp.bfloat16)


def block_levels(key, dims, split, least, high):
    factor_of = 1.0
    for position, parts in split:
        heights = jax.random.uniform(jax.random.fold_in(jax.random.fold_in(key, 6), position), (parts,), jnp.float32, least / len(split), high / len(split))
        factor_of = factor_of * jnp.repeat(jnp.exp(heights), dims[position] // parts).reshape((-1,) + (1,) * (len(dims) - 1 - position))
    return factor_of


def gaussian(own_key, extent, width, bound, shards=(), kind=jnp.bfloat16):
    result = width * jax.random.normal(own_key, extent, jnp.float32)
    if shards:
        result = result * block_levels(own_key, extent, shards, -0.22, 0.18)
    return jnp.clip(result, -bound, bound).astype(kind)


def setup_inputs(seed: int = 0, part: int = 0) -> dict:
    key_of = jax.random.split(jax.random.key(seed), 8)
    part_splits = jax.random.split(jax.random.fold_in(key_of[7], part), 8)
    return {
        "queries": draw_queries(jax.random.fold_in(jax.random.fold_in(key_of[7], part), 71), part),
        "key_cache": draw_key_cache(jax.random.fold_in(jax.random.fold_in(key_of[7], part), 71), part),
        "value_cache": gaussian(part_splits[2], (SLOTS, PAGE, KVH * DH), 1.0, 6.0, ((0, 8), (2, 2))),
        "seq_lengths": draw_seq_lengths(jax.random.fold_in(jax.random.fold_in(key_of[7], part), 71), part),
        "slot_owner": draw_slot_owner(jax.random.fold_in(jax.random.fold_in(key_of[7], part), 71), part),
        "slot_page": draw_slot_page(jax.random.fold_in(jax.random.fold_in(key_of[7], part), 71), part),
        "out_weight": gaussian(key_of[6], (HQ * DH, D), (HQ * DH) ** -0.5, 0.0625, ((0, 2), (1, 8))),
    }


neg_fill = -1e+30

def reference(queries, key_cache, value_cache, seq_lengths, slot_owner, slot_page, out_weight):
    per_group = HQ // KVH
    blocks = SLOTS // PAGE_DEV
    query_heads = queries.astype(jnp.float32).reshape(BATCH, KVH, per_group, DH)
    valid = jnp.clip(seq_lengths[slot_owner] - slot_page * PAGE, 0, PAGE).astype(jnp.int32)
    positions = jnp.arange(PAGE, dtype=jnp.int32)

    def one_block(block):
        key_tiles, value_tiles, owners, counts = block
        picked = query_heads[owners]
        key_float = key_tiles.astype(jnp.float32).reshape(PAGE_DEV, PAGE, KVH, DH)
        value_float = value_tiles.astype(jnp.float32).reshape(PAGE_DEV, PAGE, KVH, DH)
        scores = jnp.einsum('sgjd,stgd->sgjt', picked, key_float, precision=lax.Precision.HIGHEST)
        scores = scores * (1.0 / jnp.sqrt(jnp.float32(DH)))
        live = (positions[None, :] < counts[:, None])[:, None, None, :]
        scores = jnp.where(live, scores, neg_fill)
        page_peak = lax.optimization_barrier(jnp.max(scores, axis=-1))
        probs = jnp.exp(scores - page_peak[..., None]).astype(jnp.bfloat16)
        prob_float = probs.astype(jnp.float32)
        page_mass = lax.optimization_barrier(jnp.sum(prob_float, axis=-1))
        page_out = jnp.einsum('sgjt,stgd->sgjd', prob_float, value_float, precision=lax.Precision.HIGHEST)
        return (page_peak, page_mass, page_out)
    page_peak, page_mass, page_out = lax.map(one_block, (key_cache.reshape(blocks, PAGE_DEV, PAGE, KVH * DH), value_cache.reshape(blocks, PAGE_DEV, PAGE, KVH * DH), slot_owner.reshape(blocks, PAGE_DEV), valid.reshape(blocks, PAGE_DEV)))
    page_peak = page_peak.reshape(SLOTS, KVH, per_group)
    page_mass = page_mass.reshape(SLOTS, KVH, per_group)
    page_out = page_out.reshape(SLOTS, KVH, per_group, DH)
    owner_hits = slot_owner[None, :] == jnp.arange(BATCH, dtype=jnp.int32)[:, None]
    seq_peak = lax.optimization_barrier(jnp.max(jnp.where(owner_hits[:, :, None, None], page_peak[None], neg_fill), axis=1))
    factor = jnp.exp(page_peak - seq_peak[slot_owner])
    seq_mass = jax.ops.segment_sum(page_mass * factor, slot_owner, num_segments=BATCH)
    seq_out = jax.ops.segment_sum(page_out * factor[..., None], slot_owner, num_segments=BATCH)
    attention = (seq_out / seq_mass[..., None]).reshape(BATCH, HQ * DH).astype(jnp.bfloat16)
    return jnp.dot(attention, out_weight, preferred_element_type=jnp.float32).astype(jnp.bfloat16)
```

```python
import functools

import jax
import jax.numpy as jnp
from jax import lax
from jax.experimental import pallas as pl
from jax.experimental.pallas import tpu as pltpu
from jax.sharding import PartitionSpec as P

DH = 128
NEG = -1e30
MESH = pl.DeviceIdType.MESH


class Plan:
    def __init__(self, mesh_shape, q_shape, k_shape, w_shape):
        self.seq, self.sub, self.head = (mesh_shape[a] for a in ("seq", "sub", "head"))
        self.peers = self.seq * self.sub
        self.batch = q_shape[0]
        self.pages, self.page, self.width = k_shape
        self.groups = self.width // DH
        self.per_group = q_shape[1] // self.width
        self.unit_groups = 2 if self.groups % 2 == 0 else 1
        self.units = self.groups // self.unit_groups
        self.unit_heads = self.unit_groups * self.per_group
        self.unit_width = self.unit_groups * DH
        self.rows = self.batch * self.unit_heads
        self.lanes = max(128, self.rows)
        self.chunk = min(8, self.pages)
        self.chunks = self.pages // self.chunk
        self.span = self.chunk * self.page
        self.columns = w_shape[1]
        self.depth = self.unit_heads * DH


def kernel(
    pn,
    lengths, owners, numbers,
    q_ref, k_hbm, v_hbm, w_hbm,
    out_ref,
    kbuf, vbuf, wbuf, scores, qf, qb, att,
    osend, ssend, orecv, srecv, parts,
    ksem, vsem, wsem, osem_s, osem_r, ssem_s, ssem_r, psem_s, psem_r,
):
    i_seq, i_sub, i_head = (lax.axis_index(a) for a in ("seq", "sub", "head"))
    me = i_seq * pn.sub + i_sub
    n = pn.peers

    def peer_id(k):
        who = lax.rem(me + k, n)
        return {"seq": who // pn.sub, "sub": lax.rem(who, pn.sub)}

    def k_copy(u, c):
        at = (pl.ds(c * pn.chunk, pn.chunk), slice(None), pl.ds(u * pn.unit_width, pn.unit_width))
        return pltpu.make_async_copy(k_hbm.at[at], kbuf.at[at], ksem.at[u, c])

    def v_copy(u, c):
        at = (pl.ds(c * pn.chunk, pn.chunk), slice(None), pl.ds(u * pn.unit_width, pn.unit_width))
        return pltpu.make_async_copy(v_hbm.at[at], vbuf.at[at], vsem.at[u, c])

    def w_copy(u):
        at = pl.ds(u * pn.depth, pn.depth)
        return pltpu.make_async_copy(w_hbm.at[at], wbuf.at[at], wsem.at[u])

    for u in range(pn.units):
        for c in range(pn.chunks):
            k_copy(u, c).start()
        for c in range(pn.chunks):
            v_copy(u, c).start()
    for u in range(pn.units):
        w_copy(u).start()

    barrier = pltpu.get_barrier_semaphore()
    for k in range(1, n):
        pl.semaphore_signal(barrier, inc=1, device_id=peer_id(k), device_id_type=MESH)
    for k in range(1, pn.head):
        pl.semaphore_signal(
            barrier, inc=1, device_id={"head": lax.rem(i_head + k, pn.head)}, device_id_type=MESH
        )

    qf[...] = jnp.zeros_like(qf)
    for u in range(pn.units):
        for h in range(pn.unit_heads):
            g = h // pn.per_group
            col = (u * pn.unit_heads + h) * DH
            qf[u, g, pl.ds(h, pn.batch, stride=pn.unit_heads), :] = q_ref[
                :, pl.ds(col, DH)
            ].astype(jnp.float32)
    for u in range(pn.units):
        for g in range(pn.unit_groups):
            qb[u, :, pl.ds(g * DH, DH)] = qf[u, g].astype(jnp.bfloat16)
    scale = 1.0 / (DH**0.5)

    def o_copy(u, k):
        return pltpu.make_async_remote_copy(
            src_ref=osend.at[u], dst_ref=orecv.at[u, me],
            send_sem=osem_s.at[u, k], recv_sem=osem_r.at[u, k],
            device_id=peer_id(k), device_id_type=MESH,
        )

    def s_copy(u, k):
        return pltpu.make_async_remote_copy(
            src_ref=ssend.at[u], dst_ref=srecv.at[u, me],
            send_sem=ssem_s.at[u, k], recv_sem=ssem_r.at[u, k],
            device_id=peer_id(k), device_id_type=MESH,
        )

    def attend(u):
        cols = pl.ds(u * pn.unit_width, pn.unit_width)
        query = qb[u]
        spot = lax.broadcasted_iota(jnp.int32, (pn.unit_heads, pn.page), 1)

        def score_chunk(c, top):
            k_copy(u, c).wait()
            keys = kbuf[pl.ds(c * pn.chunk, pn.chunk), :, cols].reshape(pn.span, pn.unit_width)
            raw = lax.dot_general(
                query, keys, (((1,), (1,)), ((), ())), preferred_element_type=jnp.float32
            ) * scale
            pieces = []
            for p in range(pn.chunk):
                owner = owners[c * pn.chunk + p]
                number = numbers[c * pn.chunk + p]
                valid = jnp.clip(lengths[owner] - number * pn.page, 0, pn.page)
                blocks = []
                for b in range(pn.batch):
                    limit = jnp.where(owner == b, valid, 0)
                    part = raw[b * pn.unit_heads:(b + 1) * pn.unit_heads, p * pn.page:(p + 1) * pn.page]
                    blocks.append(jnp.where(spot < limit, part, NEG))
                piece = jnp.concatenate(blocks, axis=0)
                top = jnp.maximum(top, piece)
                pieces.append(piece)
            scores[c] = jnp.concatenate(pieces, axis=1)
            return top

        top = lax.fori_loop(
            0, pn.chunks, score_chunk, jnp.full((pn.rows, pn.page), NEG, jnp.float32)
        )
        peak = jnp.max(top, axis=1, keepdims=True)

        def value_chunk(c, state):
            mass, total = state
            v_copy(u, c).wait()
            probs = jnp.exp(scores[c] - peak).astype(jnp.bfloat16)
            values = vbuf[pl.ds(c * pn.chunk, pn.chunk), :, cols].reshape(pn.span, pn.unit_width)
            total = total + jnp.dot(probs, values, preferred_element_type=jnp.float32)
            pf = probs.astype(jnp.float32)
            for p in range(pn.chunk):
                mass = mass + pf[:, p * pn.page:(p + 1) * pn.page]
            return mass, total

        mass, total = lax.fori_loop(
            0, pn.chunks, value_chunk,
            (
                jnp.zeros((pn.rows, pn.page), jnp.float32),
                jnp.zeros((pn.rows, pn.unit_width), jnp.float32),
            ),
        )
        mass = jnp.sum(mass, axis=1, keepdims=True)
        level = peak + jnp.log(mass)
        blocks = []
        for b in range(pn.batch):
            for g in range(pn.unit_groups):
                r = b * pn.unit_heads + g * pn.per_group
                blocks.append(total[r:r + pn.per_group, g * DH:(g + 1) * DH])
        mine = (jnp.concatenate(blocks, axis=0) / mass).astype(jnp.bfloat16)
        line = jnp.transpose(jnp.broadcast_to(level, (pn.rows, 128)))[0:1, :]
        if pn.rows < pn.lanes:
            line = jnp.concatenate([line, jnp.zeros((1, pn.lanes - pn.rows), jnp.float32)], axis=1)
        ssend[u] = line
        osend[u] = mine
        srecv[u, me] = line
        orecv[u, me] = mine

    def send(u):
        for k in range(1, n):
            s_copy(u, k).start()
            o_copy(u, k).start()

    def merge(u):
        for k in range(1, n):
            s_copy(u, k).wait_recv()
        level = srecv[u].reshape(n, pn.lanes)
        weight = jnp.exp(level - jnp.max(level, axis=0, keepdims=True))
        weight = weight / jnp.sum(weight, axis=0, keepdims=True)
        turned = jnp.transpose(weight)
        for k in range(1, n):
            o_copy(u, k).wait_recv()
        total = None
        for s in range(n):
            term = orecv[u, s].astype(jnp.float32) * turned[0:pn.rows, s:s + 1]
            total = term if total is None else total + term
        att[u] = total
        heads = [att[u, pl.ds(h, pn.batch, stride=pn.unit_heads), :] for h in range(pn.unit_heads)]
        return jnp.concatenate(heads, axis=1).astype(jnp.bfloat16)

    for u in range(pn.units):
        attend(u)
        if u == 0:
            pl.semaphore_wait(barrier, n - 1 + pn.head - 1)
        send(u)

    total = jnp.zeros((pn.batch, pn.columns), jnp.float32)
    for u in range(pn.units):
        w_copy(u).wait()
        rows = merge(u)
        total = total + jnp.dot(
            rows, wbuf[pl.ds(u * pn.depth, pn.depth), :], preferred_element_type=jnp.float32
        )
    parts[i_head] = total

    def p_copy(k):
        return pltpu.make_async_remote_copy(
            src_ref=parts.at[i_head], dst_ref=parts.at[i_head],
            send_sem=psem_s.at[k], recv_sem=psem_r.at[k],
            device_id={"head": lax.rem(i_head + k, pn.head)}, device_id_type=MESH,
        )

    for k in range(1, pn.head):
        p_copy(k).start()
    for u in range(pn.units):
        for k in range(1, n):
            s_copy(u, k).wait_send()
            o_copy(u, k).wait_send()
    for k in range(1, pn.head):
        p_copy(k).wait()
    result = parts[0]
    for s in range(1, pn.head):
        result = result + parts[s]
    out_ref[...] = result.astype(out_ref.dtype)


def on_device(mesh_shape, queries, key_cache, value_cache, seq_lengths, slot_owner, slot_page, out_weight):
    pn = Plan(mesh_shape, queries.shape, key_cache.shape, out_weight.shape)
    smem = pl.BlockSpec(memory_space=pltpu.SMEM)
    vmem = pl.BlockSpec(memory_space=pltpu.VMEM)
    anywhere = pl.BlockSpec(memory_space=pl.ANY)
    n, u = pn.peers, pn.units
    dma = pltpu.SemaphoreType.DMA
    return pl.pallas_call(
        functools.partial(kernel, pn),
        out_shape=jax.ShapeDtypeStruct((pn.batch, pn.columns), queries.dtype),
        in_specs=[smem, smem, smem, vmem, anywhere, anywhere, anywhere],
        out_specs=vmem,
        scratch_shapes=[
            pltpu.VMEM(key_cache.shape, key_cache.dtype),
            pltpu.VMEM(value_cache.shape, value_cache.dtype),
            pltpu.VMEM(out_weight.shape, out_weight.dtype),
            pltpu.VMEM((pn.chunks, pn.rows, pn.span), jnp.float32),
            pltpu.VMEM((u, pn.unit_groups, pn.rows, DH), jnp.float32),
            pltpu.VMEM((u, pn.rows, pn.unit_width), jnp.bfloat16),
            pltpu.VMEM((u, pn.rows, DH), jnp.float32),
            pltpu.VMEM((u, pn.rows, DH), jnp.bfloat16),
            pltpu.VMEM((u, 1, pn.lanes), jnp.float32),
            pltpu.VMEM((u, n, pn.rows, DH), jnp.bfloat16),
            pltpu.VMEM((u, n, 1, pn.lanes), jnp.float32),
            pltpu.VMEM((pn.head, pn.batch, pn.columns), jnp.float32),
            dma((u, pn.chunks)), dma((u, pn.chunks)), dma((u,)),
            dma((u, n)), dma((u, n)), dma((u, n)), dma((u, n)),
            dma((pn.head,)), dma((pn.head,)),
        ],
        compiler_params=pltpu.CompilerParams(
            collective_id=0, has_side_effects=True, vmem_limit_bytes=60 * 1024 * 1024
        ),
    )(seq_lengths, slot_owner, slot_page, queries, key_cache, value_cache, out_weight)


def solution(mesh):
    in_specs = (
        P("rep", "head"),
        P(("rep", "seq", "sub"), None, "head"),
        P(("rep", "seq", "sub"), None, "head"),
        P("rep"),
        P(("rep", "seq", "sub")),
        P(("rep", "seq", "sub")),
        P("head", ("seq", "sub")),
    )
    return jax.shard_map(
        functools.partial(on_device, dict(mesh.shape)),
        mesh=mesh, in_specs=in_specs, out_specs=P("rep", ("seq", "sub")), check_vma=False,
    )
```

```python
import functools

import jax
import jax.numpy as jnp
from jax import lax
from jax.experimental import pallas as pl
from jax.experimental.pallas import tpu as pltpu
from jax.sharding import PartitionSpec as P

DH = 128
NEG = -1e30
MESH = pl.DeviceIdType.MESH


class Plan:
    def __init__(self, mesh_shape, q_shape, k_shape, w_shape):
        self.seq, self.sub, self.head = (mesh_shape[a] for a in ("seq", "sub", "head"))
        self.peers = self.seq * self.sub
        self.batch = q_shape[0]
        self.pages, self.page, self.width = k_shape
        self.groups = self.width // DH
        self.per_group = q_shape[1] // self.width
        self.unit_groups = 2 if self.groups % 2 == 0 else 1
        self.units = self.groups // self.unit_groups
        self.unit_heads = self.unit_groups * self.per_group
        self.unit_width = self.unit_groups * DH
        self.rows = self.batch * self.unit_heads
        self.lanes = max(128, self.rows)
        self.window = 5
        self.chunk = min(16, self.pages)
        self.chunks = self.pages // self.chunk
        self.span = self.chunk * self.page
        self.columns = w_shape[1]
        self.depth = self.unit_heads * DH


def kernel(
    pn,
    lengths, owners, numbers,
    q_ref, k_hbm, v_hbm, w_hbm,
    out_ref,
    kbuf, vbuf, wbuf, scores, qf, qb, att,
    probs, orecv, srecv, parts,
    ksem, vsem, wsem, osem_s, osem_r, ssem_s, ssem_r, psem_s, psem_r,
):
    i_seq, i_sub, i_head = (lax.axis_index(a) for a in ("seq", "sub", "head"))
    me = i_seq * pn.sub + i_sub
    n = pn.peers

    def k_copy(u, c):
        at = (pl.ds(c * pn.chunk, pn.chunk), slice(None), pl.ds(u * pn.unit_width, pn.unit_width))
        return pltpu.make_async_copy(k_hbm.at[at], kbuf.at[at], ksem.at[u, c])

    def v_copy(u, c):
        at = (pl.ds(c * pn.chunk, pn.chunk), slice(None), pl.ds(u * pn.unit_width, pn.unit_width))
        return pltpu.make_async_copy(v_hbm.at[at], vbuf.at[at], vsem.at[u, c])

    def w_copy(u):
        at = pl.ds(u * pn.depth, pn.depth)
        return pltpu.make_async_copy(w_hbm.at[at], wbuf.at[at], wsem.at[u])

    order = []
    for u in range(pn.units):
        order += [k_copy(u, c) for c in range(pn.chunks)]
    for u in range(pn.units):
        order += [v_copy(u, c) for c in range(pn.chunks)]
    order += [w_copy(u) for u in range(pn.units)]
    reads = pn.units * pn.chunks * 2

    for copy in order[:pn.window]:
        copy.start()

    def arrive(at):
        order[at].wait()
        if at + pn.window < reads:
            order[at + pn.window].start()
        elif at + pn.window == reads:
            for copy in order[reads:]:
                copy.start()

    barrier = pltpu.get_barrier_semaphore()
    for axis, size, index in (("seq", pn.seq, i_seq), ("sub", pn.sub, i_sub), ("head", pn.head, i_head)):
        for k in range(1, size):
            pl.semaphore_signal(
                barrier, inc=1, device_id={axis: lax.rem(index + k, size)}, device_id_type=MESH
            )

    qf[...] = jnp.zeros_like(qf)
    for u in range(pn.units):
        for h in range(pn.unit_heads):
            g = h // pn.per_group
            col = (u * pn.unit_heads + h) * DH
            qf[u, g, pl.ds(h, pn.batch, stride=pn.unit_heads), :] = q_ref[
                :, pl.ds(col, DH)
            ].astype(jnp.float32)
    for u in range(pn.units):
        for g in range(pn.unit_groups):
            qb[u, :, pl.ds(g * DH, DH)] = qf[u, g].astype(jnp.bfloat16)
    scale = 1.0 / (DH**0.5)

    def place(k_seq, k_sub):
        return lax.rem(i_seq + k_seq, pn.seq), lax.rem(i_sub + k_sub, pn.sub)

    def spot_of(k_seq, k_sub):
        a, b = place(k_seq, k_sub)
        return a * pn.sub + b

    def o_copy(u, k_seq, k_sub):
        target = place(k_seq if k_sub == 0 else 0, k_sub)
        slot = me if k_sub == 0 else spot_of(-k_seq + pn.seq, 0)
        return pltpu.make_async_remote_copy(
            src_ref=orecv.at[u, slot], dst_ref=orecv.at[u, slot],
            send_sem=osem_s.at[u, k_seq * pn.sub + k_sub],
            recv_sem=osem_r.at[u, k_seq * pn.sub + k_sub],
            device_id={"seq": target[0], "sub": target[1]}, device_id_type=MESH,
        )

    def s_copy(u, k_seq, k_sub):
        target = place(k_seq if k_sub == 0 else 0, k_sub)
        slot = me if k_sub == 0 else spot_of(-k_seq + pn.seq, 0)
        return pltpu.make_async_remote_copy(
            src_ref=srecv.at[u, slot], dst_ref=srecv.at[u, slot],
            send_sem=ssem_s.at[u, k_seq * pn.sub + k_sub],
            recv_sem=ssem_r.at[u, k_seq * pn.sub + k_sub],
            device_id={"seq": target[0], "sub": target[1]}, device_id_type=MESH,
        )

    page_spot = lax.broadcasted_iota(jnp.int32, (pn.unit_heads, pn.page), 1)
    limits = []
    for p in range(pn.pages):
        owner = owners[p]
        valid = jnp.clip(lengths[owner] - numbers[p] * pn.page, 0, pn.page)
        limits.append((owner, valid))
    tops = [jnp.full((pn.rows, pn.page), NEG, jnp.float32) for _ in range(pn.units)]
    peaks = [None] * pn.units
    masses = [jnp.zeros((pn.rows, pn.page), jnp.float32) for _ in range(pn.units)]
    totals = [jnp.zeros((pn.rows, pn.unit_width), jnp.float32) for _ in range(pn.units)]

    def tile(buffer, u, c):
        cols = pl.ds(u * pn.unit_width, pn.unit_width)
        return buffer[pl.ds(c * pn.chunk, pn.chunk), :, cols].reshape(pn.span, pn.unit_width)

    def score_dot(u, c):
        scores[u, c] = lax.dot_general(
            qb[u], tile(kbuf, u, c), (((1,), (1,)), ((), ())), preferred_element_type=jnp.float32
        )

    def post(u, c):
        for p in range(pn.chunk):
            owner, valid = limits[c * pn.chunk + p]
            at = pl.ds(p * pn.page, pn.page)
            blocks = []
            for b in range(pn.batch):
                limit = jnp.where(owner == b, valid, 0)
                rows = pl.ds(b * pn.unit_heads, pn.unit_heads)
                blocks.append(jnp.where(page_spot < limit, scores[u, c, rows, at] * scale, NEG))
            piece = jnp.concatenate(blocks, axis=0)
            tops[u] = jnp.maximum(tops[u], piece)
            scores[u, c, :, at] = piece
        if c == pn.chunks - 1:
            peaks[u] = jnp.max(tops[u], axis=1, keepdims=True)

    def soften(u, c):
        for p in range(pn.chunk):
            at = pl.ds(p * pn.page, pn.page)
            block = jnp.exp(scores[u, c, :, at] - peaks[u]).astype(jnp.bfloat16)
            probs[u, c, :, at] = block
            masses[u] = masses[u] + block.astype(jnp.float32)

    def value_dot(u, c):
        totals[u] = totals[u] + jnp.dot(
            probs[u, c], tile(vbuf, u, c), preferred_element_type=jnp.float32
        )

    def finish(u):
        mass = jnp.sum(masses[u], axis=1, keepdims=True)
        level = peaks[u] + jnp.log(mass)
        blocks = []
        for b in range(pn.batch):
            for g in range(pn.unit_groups):
                r = b * pn.unit_heads + g * pn.per_group
                blocks.append(totals[u][r:r + pn.per_group, g * DH:(g + 1) * DH])
        mine = (jnp.concatenate(blocks, axis=0) / mass).astype(jnp.bfloat16)
        line = jnp.transpose(jnp.broadcast_to(level, (pn.rows, 128)))[0:1, :]
        if pn.rows < pn.lanes:
            line = jnp.concatenate([line, jnp.zeros((1, pn.lanes - pn.rows), jnp.float32)], axis=1)
        srecv[u, me] = line
        orecv[u, me] = mine

    def send(u):
        if u == 0:
            pl.semaphore_wait(barrier, pn.seq + pn.sub + pn.head - 3)
        for k in range(1, pn.seq):
            s_copy(u, k, 0).start()
            o_copy(u, k, 0).start()
        for k in range(1, pn.sub):
            s_copy(u, 0, k).start()
            o_copy(u, 0, k).start()

    def relay(u):
        for k in range(1, pn.seq):
            s_copy(u, k, 0).wait_recv()
            for j in range(1, pn.sub):
                s_copy(u, k, j).start()
            o_copy(u, k, 0).wait_recv()
            for j in range(1, pn.sub):
                o_copy(u, k, j).start()

    def merge(u):
        for k in range(pn.seq):
            for j in range(1, pn.sub):
                s_copy(u, k, j).wait_recv()
                o_copy(u, k, j).wait_recv()
        level = srecv[u].reshape(n, pn.lanes)
        weight = jnp.exp(level - jnp.max(level, axis=0, keepdims=True))
        weight = weight / jnp.sum(weight, axis=0, keepdims=True)
        turned = jnp.transpose(weight)
        total = None
        for s in range(n):
            term = orecv[u, s].astype(jnp.float32) * turned[0:pn.rows, s:s + 1]
            total = term if total is None else total + term
        att[u] = total
        heads = [att[u, pl.ds(h, pn.batch, stride=pn.unit_heads), :] for h in range(pn.unit_heads)]
        return jnp.concatenate(heads, axis=1).astype(jnp.bfloat16)

    soften_at = {}
    for u in range(pn.units):
        for c in range(pn.chunks):
            step = min((u + 1) * pn.chunks + 1 + c, (pn.units + u) * pn.chunks + c)
            soften_at.setdefault(step, []).append((u, c))
    for step in range(2 * pn.units * pn.chunks):
        arrive(step)
        u, c = divmod(step, pn.chunks)
        if 1 <= step <= pn.units * pn.chunks:
            post(*divmod(step - 1, pn.chunks))
        if u < pn.units:
            score_dot(u, c)
        for item in soften_at.get(step, ()):
            soften(*item)
        if u >= pn.units:
            if c == 0 and u > pn.units:
                finish(u - pn.units - 1)
            value_dot(u - pn.units, c)
            if c == 0 and u > pn.units:
                send(u - pn.units - 1)
    finish(pn.units - 1)
    send(pn.units - 1)

    total = jnp.zeros((pn.batch, pn.columns), jnp.float32)
    relay(0)
    for u in range(pn.units):
        order[reads + u].wait()
        if u > 0:
            relay(u)
        rows = merge(u)
        total = total + jnp.dot(
            rows, wbuf[pl.ds(u * pn.depth, pn.depth), :], preferred_element_type=jnp.float32
        )
    parts[i_head] = total

    def p_copy(k):
        return pltpu.make_async_remote_copy(
            src_ref=parts.at[i_head], dst_ref=parts.at[i_head],
            send_sem=psem_s.at[k], recv_sem=psem_r.at[k],
            device_id={"head": lax.rem(i_head + k, pn.head)}, device_id_type=MESH,
        )

    for k in range(1, pn.head):
        p_copy(k).start()
    for u in range(pn.units):
        for k in range(1, n):
            s_copy(u, *divmod(k, pn.sub)).wait_send()
            o_copy(u, *divmod(k, pn.sub)).wait_send()
    for k in range(1, pn.head):
        p_copy(k).wait()
    result = parts[0]
    for s in range(1, pn.head):
        result = result + parts[s]
    out_ref[...] = result.astype(out_ref.dtype)


def on_device(mesh_shape, queries, key_cache, value_cache, seq_lengths, slot_owner, slot_page, out_weight):
    pn = Plan(mesh_shape, queries.shape, key_cache.shape, out_weight.shape)
    smem = pl.BlockSpec(memory_space=pltpu.SMEM)
    vmem = pl.BlockSpec(memory_space=pltpu.VMEM)
    anywhere = pl.BlockSpec(memory_space=pl.ANY)
    n, u = pn.peers, pn.units
    dma = pltpu.SemaphoreType.DMA
    return pl.pallas_call(
        functools.partial(kernel, pn),
        out_shape=jax.ShapeDtypeStruct((pn.batch, pn.columns), queries.dtype),
        in_specs=[smem, smem, smem, vmem, anywhere, anywhere, anywhere],
        out_specs=vmem,
        scratch_shapes=[
            pltpu.VMEM(key_cache.shape, key_cache.dtype),
            pltpu.VMEM(value_cache.shape, value_cache.dtype),
            pltpu.VMEM(out_weight.shape, out_weight.dtype),
            pltpu.VMEM((u, pn.chunks, pn.rows, pn.span), jnp.float32),
            pltpu.VMEM((u, pn.unit_groups, pn.rows, DH), jnp.float32),
            pltpu.VMEM((u, pn.rows, pn.unit_width), jnp.bfloat16),
            pltpu.VMEM((u, pn.rows, DH), jnp.float32),
            pltpu.VMEM((u, pn.chunks, pn.rows, pn.span), jnp.bfloat16),
            pltpu.VMEM((u, n, pn.rows, DH), jnp.bfloat16),
            pltpu.VMEM((u, n, 1, pn.lanes), jnp.float32),
            pltpu.VMEM((pn.head, pn.batch, pn.columns), jnp.float32),
            dma((u, pn.chunks)), dma((u, pn.chunks)), dma((u,)),
            dma((u, n)), dma((u, n)), dma((u, n)), dma((u, n)),
            dma((pn.head,)), dma((pn.head,)),
        ],
        compiler_params=pltpu.CompilerParams(
            collective_id=0, has_side_effects=True, vmem_limit_bytes=60 * 1024 * 1024
        ),
    )(seq_lengths, slot_owner, slot_page, queries, key_cache, value_cache, out_weight)


def solution(mesh):
    in_specs = (
        P("rep", "head"),
        P(("rep", "seq", "sub"), None, "head"),
        P(("rep", "seq", "sub"), None, "head"),
        P("rep"),
        P(("rep", "seq", "sub")),
        P(("rep", "seq", "sub")),
        P("head", ("seq", "sub")),
    )
    return jax.shard_map(
        functools.partial(on_device, dict(mesh.shape)),
        mesh=mesh, in_specs=in_specs, out_specs=P("rep", ("seq", "sub")), check_vma=False,
    )
```

```python
import functools

import jax
import jax.numpy as jnp
from jax import lax
from jax.experimental import pallas as pl
from jax.experimental.pallas import tpu as pltpu
from jax.sharding import PartitionSpec as P

DH = 128
NEG = -1e30
MESH = pl.DeviceIdType.MESH


class Plan:
    def __init__(self, mesh_shape, q_shape, k_shape, w_shape):
        self.seq, self.sub, self.head = (mesh_shape[a] for a in ("seq", "sub", "head"))
        self.peers = self.seq * self.sub
        self.batch = q_shape[0]
        self.pages, self.page, self.width = k_shape
        self.groups = self.width // DH
        self.per_group = q_shape[1] // self.width
        self.unit_groups = 2 if self.groups % 2 == 0 else 1
        self.units = self.groups // self.unit_groups
        self.unit_heads = self.unit_groups * self.per_group
        self.unit_width = self.unit_groups * DH
        self.rows = self.batch * self.unit_heads
        self.group_rows = self.batch * self.per_group
        self.lanes = max(128, self.group_rows)
        self.window = 5
        self.chunk = min(16, self.pages)
        self.chunks = self.pages // self.chunk
        self.span = self.chunk * self.page
        self.columns = w_shape[1]
        self.depth = self.per_group * DH
        self.relayed = self.groups // 2
        self.value_chunk = min(32, self.pages)
        self.value_chunks = self.pages // self.value_chunk
        self.value_span = self.value_chunk * self.page


def kernel(
    pn,
    lengths, owners, numbers,
    q_ref, k_hbm, v_hbm, w_hbm,
    out_ref,
    kbuf, vbuf, wbuf, scores, qf, qb, att,
    probs, orecv, srecv, parts,
    ksem, vsem, wsem, osem_s, osem_r, ssem_s, ssem_r, psem_s, psem_r,
):
    i_seq, i_sub, i_head = (lax.axis_index(a) for a in ("seq", "sub", "head"))
    me = i_seq * pn.sub + i_sub
    n = pn.peers

    def k_copy(u, c):
        at = (pl.ds(c * pn.chunk, pn.chunk), slice(None), pl.ds(u * pn.unit_width, pn.unit_width))
        return pltpu.make_async_copy(k_hbm.at[at], kbuf.at[at], ksem.at[u, c])

    def v_copy(u, c):
        at = (pl.ds(c * pn.value_chunk, pn.value_chunk), slice(None), pl.ds(u * DH, DH))
        return pltpu.make_async_copy(v_hbm.at[at], vbuf.at[at], vsem.at[u, c])

    def w_copy(u):
        at = pl.ds(u * pn.depth, pn.depth)
        return pltpu.make_async_copy(w_hbm.at[at], wbuf.at[at], wsem.at[u])

    order = []
    for u in range(pn.units):
        order += [k_copy(u, c) for c in range(pn.chunks)]
    for g in range(pn.groups):
        order += [v_copy(g, c) for c in range(pn.value_chunks)]
    order += [w_copy(g) for g in range(pn.groups)]
    score_steps = pn.units * pn.chunks
    reads = score_steps + pn.groups * pn.value_chunks

    for copy in order[:pn.window]:
        copy.start()

    def arrive(at):
        order[at].wait()
        if at + pn.window < reads:
            order[at + pn.window].start()
        elif at + pn.window == reads:
            for copy in order[reads:]:
                copy.start()

    barrier = pltpu.get_barrier_semaphore()
    for k in range(1, n):
        k_seq, k_sub = divmod(k, pn.sub)
        who = {"seq": lax.rem(i_seq + k_seq, pn.seq), "sub": lax.rem(i_sub + k_sub, pn.sub)}
        pl.semaphore_signal(barrier, inc=1, device_id=who, device_id_type=MESH)
    for k in range(1, pn.head):
        who = {"head": lax.rem(i_head + k, pn.head)}
        pl.semaphore_signal(barrier, inc=1, device_id=who, device_id_type=MESH)

    qf[...] = jnp.zeros_like(qf)
    for u in range(pn.units):
        for h in range(pn.unit_heads):
            g = h // pn.per_group
            col = (u * pn.unit_heads + h) * DH
            qf[u, g, pl.ds(g * pn.group_rows + h % pn.per_group, pn.batch, stride=pn.per_group), :] = q_ref[
                :, pl.ds(col, DH)
            ].astype(jnp.float32)
    for u in range(pn.units):
        for g in range(pn.unit_groups):
            qb[u, :, pl.ds(g * DH, DH)] = qf[u, g].astype(jnp.bfloat16)
    scale = 1.0 / (DH**0.5)

    def remote(ref, g, k, send_sem, recv_sem):
        k_seq, k_sub = divmod(k, pn.sub)
        hop, slot = k_seq, me
        if g < pn.relayed and k_sub > 0:
            hop = 0
            if k_seq > 0:
                slot = lax.rem(i_seq + pn.seq - k_seq, pn.seq) * pn.sub + i_sub
        return pltpu.make_async_remote_copy(
            src_ref=ref.at[g, slot], dst_ref=ref.at[g, slot],
            send_sem=send_sem.at[g, k], recv_sem=recv_sem.at[g, k],
            device_id={
                "seq": lax.rem(i_seq + hop, pn.seq),
                "sub": lax.rem(i_sub + k_sub, pn.sub),
            },
            device_id_type=MESH,
        )

    def o_copy(g, k):
        return remote(orecv, g, k, osem_s, osem_r)

    def s_copy(g, k):
        return remote(srecv, g, k, ssem_s, ssem_r)

    page_spot = lax.broadcasted_iota(jnp.int32, (pn.per_group, pn.page), 1)
    limits = []
    for p in range(pn.pages):
        owner = owners[p]
        valid = jnp.clip(lengths[owner] - numbers[p] * pn.page, 0, pn.page)
        limits.append((owner, valid))
    tops = [jnp.full((pn.rows, pn.page), NEG, jnp.float32) for _ in range(pn.units)]
    peaks = [None] * pn.units
    masses = [jnp.zeros((pn.group_rows, pn.page), jnp.float32) for _ in range(pn.groups)]
    totals = [jnp.zeros((pn.group_rows, DH), jnp.float32) for _ in range(pn.groups)]

    def score_dot(u, c):
        cols = pl.ds(u * pn.unit_width, pn.unit_width)
        keys = kbuf[pl.ds(c * pn.chunk, pn.chunk), :, cols].reshape(pn.span, pn.unit_width)
        scores[u, c] = lax.dot_general(
            qb[u], keys, (((1,), (1,)), ((), ())), preferred_element_type=jnp.float32
        )

    def post(u, c):
        for p in range(pn.chunk):
            owner, valid = limits[c * pn.chunk + p]
            at = pl.ds(p * pn.page, pn.page)
            blocks = []
            live = [page_spot < jnp.where(owner == b, valid, 0) for b in range(pn.batch)]
            for r in range(pn.unit_groups * pn.batch):
                rows = pl.ds(r * pn.per_group, pn.per_group)
                blocks.append(jnp.where(live[r % pn.batch], scores[u, c, rows, at] * scale, NEG))
            piece = jnp.concatenate(blocks, axis=0)
            tops[u] = jnp.maximum(tops[u], piece)
            scores[u, c, :, at] = piece
        if c == pn.chunks - 1:
            peaks[u] = jnp.max(tops[u], axis=1, keepdims=True)

    def soften(g, c):
        u, part = divmod(g, pn.unit_groups)
        rows = slice(part * pn.group_rows, (part + 1) * pn.group_rows)
        peak = peaks[u][rows]
        for p in range(pn.value_chunk):
            from_chunk, spot = divmod(c * pn.value_chunk + p, pn.chunk)
            block = jnp.exp(scores[u, from_chunk, rows, pl.ds(spot * pn.page, pn.page)] - peak)
            block = block.astype(jnp.bfloat16)
            probs[g, c, :, pl.ds(p * pn.page, pn.page)] = block
            masses[g] = masses[g] + block.astype(jnp.float32)

    def value_dot(g, c):
        values = vbuf[pl.ds(c * pn.value_chunk, pn.value_chunk), :, pl.ds(g * DH, DH)]
        totals[g] = totals[g] + jnp.dot(
            probs[g, c], values.reshape(pn.value_span, DH), preferred_element_type=jnp.float32
        )

    def finish(g):
        u, part = divmod(g, pn.unit_groups)
        mass = jnp.sum(masses[g], axis=1, keepdims=True)
        level = peaks[u][part * pn.group_rows:(part + 1) * pn.group_rows] + jnp.log(mass)
        line = jnp.transpose(jnp.broadcast_to(level, (pn.group_rows, 128)))[0:1, :]
        if pn.group_rows < pn.lanes:
            pad = jnp.zeros((1, pn.lanes - pn.group_rows), jnp.float32)
            line = jnp.concatenate([line, pad], axis=1)
        srecv[g, me] = line
        orecv[g, me] = (totals[g] / mass).astype(jnp.bfloat16)

    def send(u):
        if u == 0:
            pl.semaphore_wait(barrier, n - 1 + pn.head - 1)
        for k in [*range(pn.sub, n), *range(1, pn.sub)]:
            if k < pn.sub or u >= pn.relayed or k % pn.sub == 0:
                s_copy(u, k).start()
                o_copy(u, k).start()

    def relay(u):
        for k in range(pn.sub, n, pn.sub):
            s_copy(u, k).wait_recv()
            o_copy(u, k).wait_recv()
            for j in range(1, pn.sub):
                s_copy(u, k + j).start()
                o_copy(u, k + j).start()

    def merge(u):
        for k in range(1, n):
            if u >= pn.relayed or k % pn.sub > 0:
                s_copy(u, k).wait_recv()
                o_copy(u, k).wait_recv()
        level = srecv[u].reshape(n, pn.lanes)
        weight = jnp.exp(level - jnp.max(level, axis=0, keepdims=True))
        weight = weight / jnp.sum(weight, axis=0, keepdims=True)
        turned = jnp.transpose(weight)
        total = None
        for s in range(n):
            term = orecv[u, s].astype(jnp.float32) * turned[0:pn.group_rows, s:s + 1]
            total = term if total is None else total + term
        att[u] = total
        heads = [att[u, pl.ds(h, pn.batch, stride=pn.per_group), :] for h in range(pn.per_group)]
        return jnp.concatenate(heads, axis=1).astype(jnp.bfloat16)

    soften_at = {}
    for g in range(pn.groups):
        for c in range(pn.value_chunks):
            needed = score_steps + g * pn.value_chunks + c
            ready = (g // pn.unit_groups + 1) * pn.chunks + 1
            soften_at.setdefault(max(ready, needed - 1) if ready <= needed else needed, []).append((g, c))
    for step in range(reads):
        arrive(step)
        if 1 <= step <= score_steps:
            post(*divmod(step - 1, pn.chunks))
        if step < score_steps:
            score_dot(*divmod(step, pn.chunks))
        for item in soften_at.get(step, ()):
            soften(*item)
        if step >= score_steps:
            g, c = divmod(step - score_steps, pn.value_chunks)
            if c == 0 and g > 0:
                finish(g - 1)
            value_dot(g, c)
            if c == 0 and g > 0:
                send(g - 1)
    finish(pn.groups - 1)
    send(pn.groups - 1)

    for g in range(pn.relayed):
        relay(g)
    total = jnp.zeros((pn.batch, pn.columns), jnp.float32)
    for g in range(pn.groups):
        order[reads + g].wait()
        rows = merge(g)
        total = total + jnp.dot(
            rows, wbuf[pl.ds(g * pn.depth, pn.depth), :], preferred_element_type=jnp.float32
        )
    parts[i_head] = total

    def p_copy(k):
        return pltpu.make_async_remote_copy(
            src_ref=parts.at[i_head], dst_ref=parts.at[i_head],
            send_sem=psem_s.at[k], recv_sem=psem_r.at[k],
            device_id={"head": lax.rem(i_head + k, pn.head)}, device_id_type=MESH,
        )

    for k in range(1, pn.head):
        p_copy(k).start()
    for u in range(pn.groups):
        for k in range(1, n):
            s_copy(u, k).wait_send()
            o_copy(u, k).wait_send()
    for k in range(1, pn.head):
        p_copy(k).wait()
    result = parts[0]
    for s in range(1, pn.head):
        result = result + parts[s]
    out_ref[...] = result.astype(out_ref.dtype)


def on_device(mesh_shape, queries, key_cache, value_cache, seq_lengths, slot_owner, slot_page, out_weight):
    pn = Plan(mesh_shape, queries.shape, key_cache.shape, out_weight.shape)
    smem = pl.BlockSpec(memory_space=pltpu.SMEM)
    vmem = pl.BlockSpec(memory_space=pltpu.VMEM)
    anywhere = pl.BlockSpec(memory_space=pl.ANY)
    n, u, g = pn.peers, pn.units, pn.groups
    dma = pltpu.SemaphoreType.DMA
    return pl.pallas_call(
        functools.partial(kernel, pn),
        out_shape=pltpu.VMEM((pn.batch, pn.columns), queries.dtype),
        in_specs=[smem, smem, smem, vmem, anywhere, anywhere, anywhere],
        out_specs=vmem,
        scratch_shapes=[
            pltpu.VMEM(key_cache.shape, key_cache.dtype),
            pltpu.VMEM(value_cache.shape, value_cache.dtype),
            pltpu.VMEM(out_weight.shape, out_weight.dtype),
            pltpu.VMEM((u, pn.chunks, pn.rows, pn.span), jnp.float32),
            pltpu.VMEM((u, pn.unit_groups, pn.rows, DH), jnp.float32),
            pltpu.VMEM((u, pn.rows, pn.unit_width), jnp.bfloat16),
            pltpu.VMEM((g, pn.group_rows, DH), jnp.float32),
            pltpu.VMEM((g, pn.value_chunks, pn.group_rows, pn.value_span), jnp.bfloat16),
            pltpu.VMEM((g, n, pn.group_rows, DH), jnp.bfloat16),
            pltpu.VMEM((g, n, 1, pn.lanes), jnp.float32),
            pltpu.VMEM((pn.head, pn.batch, pn.columns), jnp.float32),
            dma((u, pn.chunks)), dma((g, pn.value_chunks)), dma((g,)),
            dma((g, n)), dma((g, n)), dma((g, n)), dma((g, n)),
            dma((pn.head,)), dma((pn.head,)),
        ],
        compiler_params=pltpu.CompilerParams(
            collective_id=0, has_side_effects=True, vmem_limit_bytes=60 * 1024 * 1024
        ),
    )(seq_lengths, slot_owner, slot_page, queries, key_cache, value_cache, out_weight)


def solution(mesh):
    in_specs = (
        P("rep", "head"),
        P(("rep", "seq", "sub"), None, "head"),
        P(("rep", "seq", "sub"), None, "head"),
        P("rep"),
        P(("rep", "seq", "sub")),
        P(("rep", "seq", "sub")),
        P("head", ("seq", "sub")),
    )
    return jax.shard_map(
        functools.partial(on_device, dict(mesh.shape)),
        mesh=mesh, in_specs=in_specs, out_specs=P("rep", ("seq", "sub")), check_vma=False,
    )
```
